768 devices in a mesh: dp: 48 (over z, x_hi, core), tensor: 16 (over y, x_lo).
Axes of the slice: x: 4 (x_hi: 2, x_lo: 2; x = x_hi * 2 + x_lo), y: 8, z: 12, core: 2. Of those that a mesh axis runs over, the one named last changes fastest.
Arguments:
- grads: bfloat16 [48, 384, 28672], P('dp', None, 'tensor'), may hold values from -900 to 900
- params: float32 [384, 28672], P('dp', 'tensor'), may hold values from -6 to 6
- moment: float32 [384, 28672], P('dp', 'tensor'), may hold values from -0.6 to 0.6
- variance: float32 [384, 28672], P('dp', 'tensor'), may hold values from 0.01 to 1
- save_owner: int32 [48, 16], P('dp'), may hold values from 0 to 15, each once within a row
Outputs:
- fresh_params: float32 [384, 28672], P('dp', 'tensor')
- moment_next: float32 [384, 28672], P('dp', 'tensor')
- variance_next: float32 [384, 28672], P('dp', 'tensor')
- save_groups: bfloat16 [6144, 1792], P(('dp', 'tensor'))
The draws below stay inside these ranges and needn't reach their ends.
Inputs may be any that keep to these rules, and one draw needn't show every extreme that they name: Each row of save_owner names every index of 0 to 15 once.
All inputs are finite; a program needn't handle non-finite values.
Results may differ from the reference program's by a relative error of at most 0.001.
Values may be sent and summed in bfloat16 or wider, within the bound.
No kernel may reach another device: no remote copies, remote signals or barrier semaphores. Data moves between devices by JAX's collectives and lax.ppermute only.
A program may use at most 32 MiB of HBM per device.

```python
import math
import jax
import jax.numpy as jnp
from jax import lax

FF = 28672
OWN_ROWS = 8
ROWS = 384
N_DP = 48
N_TENSOR = 16


def draw_grads(key, part):
    keys = jax.random.split(key, 3)
    row_pos = jnp.arange(ROWS, dtype=jnp.float32) / ROWS
    col_pos = jnp.arange(FF, dtype=jnp.float32) / FF
    row_scale = jnp.exp(math.log(3.0) * row_pos + jax.random.uniform(keys[0], (ROWS,), minval=0.0, maxval=math.log(10.0 / 3.0)))
    col_scale = jnp.exp(math.log(3.0) * col_pos + jax.random.uniform(keys[1], (FF,), minval=0.0, maxval=math.log(10.0 / 3.0)))
    own_part = jax.random.truncated_normal(keys[2], -4.0, 4.0, (N_DP, ROWS, FF), jnp.float32)
    base = own_part
    values = base * row_scale[None, :, None] * col_scale[None, None, :]
    return values.astype(jnp.bfloat16)


def levels(stream_key, extent, pieces, low, largest):
    gain = 1.0
    for dim, shards_of in pieces:
        heights = jax.random.uniform(jax.random.fold_in(jax.random.fold_in(stream_key, 6), dim), (shards_of,), jnp.float32, low / len(pieces), largest / len(pieces))
        gain = gain * jnp.repeat(jnp.exp(heights), extent[dim] // shards_of).reshape((-1,) + (1,) * (len(extent) - 1 - dim))
    return gain


def gaussian(stream_key, dims, width, bound, pieces=(), kind=jnp.bfloat16):
    gain = levels(stream_key, dims, pieces, -0.22, 0.18) if pieces else 1.0
    array = jax.random.normal(stream_key, dims, jnp.float32) * width * gain
    return jnp.minimum(jnp.maximum(array, -bound), bound).astype(kind)


def setup_inputs(seed: int = 0) -> dict:
    key_list = jax.random.split(jax.random.key(seed), 6)
    return {
        "grads": draw_grads(jax.random.fold_in(key_list[5], 71), 0),
        "params": gaussian(key_list[1], (ROWS, FF), 1.0, 6.0, ((0, 48), (1, 16)), jnp.float32),
        "moment": gaussian(key_list[2], (ROWS, FF), 0.1, 0.6, ((0, 48), (1, 16)), jnp.float32),
        "variance": jnp.clip(jnp.exp(math.log(1.0) - 4.6051702 * jax.random.uniform(key_list[3], (ROWS, FF), jnp.float32) ** levels(key_list[3], (ROWS, FF), ((0, 48), (1, 16)), -0.2, 0.2)), 0.01, 1.0),
        "save_owner": jax.vmap(lambda own: jax.random.permutation(own, N_TENSOR))(jax.random.split(key_list[4], N_DP)).reshape((N_DP, N_TENSOR)).astype(jnp.int32),
    }


learn_rate = 0.05
beta_first = 0.9
beta_second = 0.999
adam_step = 1000.0
adam_eps = 1e-08
norm_eps = 1e-06

def adam_update(summed, params, moment, variance, clip_scale):
    scaled = clip_scale * summed
    moment_next = beta_first * moment + (1.0 - beta_first) * scaled
    variance_next = beta_second * variance + (1.0 - beta_second) * scaled * scaled
    first_fix = 1.0 - beta_first ** adam_step
    second_fix = 1.0 - beta_second ** adam_step
    update = moment_next / first_fix / (jnp.sqrt(variance_next / second_fix) + adam_eps)
    return (params - learn_rate * update, moment_next, variance_next)

def reference(grads, params, moment, variance, save_owner):

    def accumulate(replica, carry):
        return carry + grads[replica].astype(jnp.float32)
    summed = lax.fori_loop(0, N_DP, accumulate, jnp.zeros(params.shape, jnp.float32))
    squares = jnp.sum(summed * summed)
    norm_limit = math.sqrt(float(ROWS * FF))
    clip_scale = jnp.minimum(1.0, norm_limit / (jnp.sqrt(squares) + norm_eps))
    fresh_params, moment_next, variance_next = adam_update(summed, params, moment, variance, clip_scale)
    saved_rows = fresh_params.astype(jnp.bfloat16)
    blocks = saved_rows.reshape(N_DP, N_TENSOR, OWN_ROWS * FF // N_TENSOR)
    inverse = jnp.argsort(save_owner, axis=1).astype(jnp.int32)
    groups = jnp.take_along_axis(blocks, inverse[:, :, None], axis=1)
    return (fresh_params, moment_next, variance_next, groups.reshape(ROWS * N_TENSOR, FF // N_TENSOR))
```

```python
import math

import jax
import jax.numpy as jnp
from jax import lax
from jax.sharding import Mesh
from jax.sharding import PartitionSpec as P

TENSOR = ("tensor_0", "tensor_1")
DP = ("dp_0", "dp_1", "dp_2")
DP_TENSOR = ("dp_0", "dp_1", "dp_2", "tensor_0", "tensor_1")
SWAP = ((0, 1), (1, 0))
LANES = 128

learn_rate = 0.05
beta_first = 0.9
beta_second = 0.999
adam_step = 1000.0
adam_eps = 1e-08
norm_eps = 1e-06

SPREAD = 1024.0


def encode(value):
    root = jnp.sqrt(jnp.abs(value)) * SPREAD
    return jnp.where(value < 0.0, -root, root).astype(jnp.float16)


def decode(code):
    root = code.astype(jnp.float32) * (1.0 / SPREAD)
    return root * jnp.abs(root)


def adam_update(summed, params, moment, variance, clip_scale):
    scaled = clip_scale * summed
    moment_next = beta_first * moment + (1.0 - beta_first) * scaled
    variance_next = beta_second * variance + (1.0 - beta_second) * scaled * scaled
    first_fix = 1.0 - beta_first**adam_step
    second_fix = 1.0 - beta_second**adam_step
    update = moment_next / first_fix / (jnp.sqrt(variance_next / second_fix) + adam_eps)
    return (params - learn_rate * update, moment_next, variance_next)


def exchange(array, axes):
    return lax.all_to_all(array, axes, split_axis=0, concat_axis=0, tiled=True)


def total_over(value, axes):
    count = lax.axis_size(axes)
    copies = jnp.broadcast_to(value, (count, 1, LANES))
    return jnp.sum(exchange(copies, axes)[:, 0, 0])


def shards(grads, params, moment, variance, save_owner):
    own_rows, width = params.shape
    tensor_count = lax.axis_size(TENSOR)
    far, core = lax.axis_index("dp_1"), lax.axis_index("dp_2")
    tensor_place = lax.axis_index(TENSOR)
    halves = tensor_count // own_rows
    entries = grads.shape[1] * width * tensor_count
    norm_limit = math.sqrt(float(entries))

    owners = save_owner[0]
    row_owner = jnp.take(owners.reshape(own_rows, halves), tensor_place // own_rows, axis=1)
    slots = jnp.arange(tensor_count, dtype=jnp.int32)
    goes = row_owner[None, :] == slots[:, None]
    source_row = jnp.sum(jnp.where(goes, jnp.arange(own_rows)[None, :], 0), axis=1)
    own_group = jnp.sum(jnp.where(owners == tensor_place, slots, 0))
    first_sender = (own_group % halves) * own_rows

    def pack(array):
        return jnp.take(array, source_row, axis=0)

    def unpack(array):
        return lax.dynamic_slice_in_dim(array, first_sender, own_rows, axis=0)

    state = jnp.stack([params, moment, variance], axis=1)
    state = exchange(pack(state), TENSOR)

    by_place = grads[0].reshape(
        lax.axis_size("dp_0"), lax.axis_size("dp_1"), lax.axis_size("dp_2"), own_rows, width
    )
    kept = lax.dynamic_index_in_dim(by_place, core, axis=2, keepdims=False)
    sent = lax.dynamic_index_in_dim(by_place, 1 - core, axis=2, keepdims=False)
    arrived = lax.ppermute(sent, "dp_2", SWAP)
    pair = kept.astype(jnp.float32) + arrived.astype(jnp.float32)
    kept = lax.dynamic_index_in_dim(pair, far, axis=1, keepdims=False)
    sent = lax.dynamic_index_in_dim(pair, 1 - far, axis=1, keepdims=False)
    four = kept + decode(lax.ppermute(encode(sent), "dp_1", SWAP))
    codes, state = lax.optimization_barrier((encode(four), state))
    state = unpack(state)
    summed = jnp.sum(decode(exchange(codes, "dp_0")), axis=0)

    squares = jnp.sum(summed * summed)
    pieces = jnp.concatenate(
        [pack(summed)[:, None, :], jnp.broadcast_to(squares, (tensor_count, 1, LANES))], axis=2
    )
    received = exchange(pieces, TENSOR)
    group_summed = unpack(received[:, 0, :width])
    squares = jnp.sum(received[:, 0, width])
    squares = total_over(squares, ("dp_1", "dp_2"))
    squares = total_over(squares, "dp_0")
    clip_scale = jnp.minimum(1.0, norm_limit / (jnp.sqrt(squares) + norm_eps))

    fresh_params, moment_next, variance_next = adam_update(
        summed, params, moment, variance, clip_scale
    )
    groups = adam_update(group_summed, state[:, 0], state[:, 1], state[:, 2], clip_scale)[0]
    return (fresh_params, moment_next, variance_next, groups.astype(jnp.bfloat16))


def solution(mesh):
    torus = Mesh(
        mesh.devices.reshape(12, 2, 2, 8, 2), ("dp_0", "dp_1", "dp_2", "tensor_0", "tensor_1")
    )
    return jax.shard_map(
        shards,
        mesh=torus,
        in_specs=(P(DP, None, TENSOR), P(DP, TENSOR), P(DP, TENSOR), P(DP, TENSOR), P(DP, None)),
        out_specs=(P(DP, TENSOR), P(DP, TENSOR), P(DP, TENSOR), P(DP_TENSOR, None)),
        check_vma=False,
    )
```

```python
import functools
import math

import jax
import jax.numpy as jnp
from jax import lax
from jax.experimental import pallas as pl
from jax.experimental.pallas import tpu as pltpu
from jax.sharding import Mesh
from jax.sharding import PartitionSpec as P


TENSOR = ("tensor_0", "tensor_1")
DP = ("dp_0", "dp_1", "dp_2")
DP_TENSOR = ("dp_0", "dp_1", "dp_2", "tensor_0", "tensor_1")
SWAP = ((0, 1), (1, 0))
LANES = 128

learn_rate = 0.05
beta_first = 0.9
beta_second = 0.999
adam_step = 1000.0
adam_eps = 1e-08
norm_eps = 1e-06

SPREAD = 16.0


def encode(value):
    return (value * SPREAD).astype(jnp.float16)


def decode(code):
    return code.astype(jnp.float32) * (1.0 / SPREAD)


def adam_update(summed, params, moment, variance, clip_scale):
    scaled = clip_scale * summed
    moment_next = beta_first * moment + (1.0 - beta_first) * scaled
    variance_next = beta_second * variance + (1.0 - beta_second) * scaled * scaled
    first_fix = 1.0 - beta_first**adam_step
    second_fix = 1.0 - beta_second**adam_step
    update = moment_next / first_fix / (jnp.sqrt(variance_next / second_fix) + adam_eps)
    return (params - learn_rate * update, moment_next, variance_next)


def exchange(array, axes):
    return lax.all_to_all(array, axes, split_axis=0, concat_axis=0, tiled=True)


def in_vmem():
    return pl.BlockSpec(memory_space=pltpu.VMEM)


def keep(array):
    return pltpu.with_memory_space_constraint(array, pltpu.VMEM)


def in_smem():
    return pl.BlockSpec(memory_space=pltpu.SMEM)


def pack_state(owners, params, moment, variance, out):
    own_rows, width = params.shape
    halves = owners.shape[1] // own_rows
    half = lax.axis_index(TENSOR) // own_rows
    for row in range(own_rows):
        slot = owners[0, row * halves + half]
        for place, array in enumerate((params, moment, variance)):
            out[slot, :, place * width : (place + 1) * width] = array[row : row + 1, :]


def pack_summed(owners, summed, out):
    own_rows, width = summed.shape
    halves = owners.shape[1] // own_rows
    half = lax.axis_index(TENSOR) // own_rows
    squares = jnp.zeros((own_rows, LANES), jnp.float32)
    for start in range(0, width, LANES):
        tile = summed[:, start : start + LANES]
        squares = squares + tile * tile
    squares = jnp.sum(squares, axis=0, keepdims=True)
    for slot in range(out.shape[0]):
        out[slot, :, width:] = squares
    for row in range(own_rows):
        slot = owners[0, row * halves + half]
        out[slot, :, :width] = summed[row : row + 1, :]


def finish(norm_limit, owners, squares, received, state, summed, params, moment, variance,
           fresh_out, moment_out, variance_out, groups_out):
    own_rows, width = params.shape
    tensor_count = owners.shape[1]
    halves = tensor_count // own_rows
    place = lax.axis_index(TENSOR)
    first = jnp.int32(0)
    for group in range(tensor_count):
        first = jnp.where(owners[0, group] == place, group % halves * own_rows, first)
    norm = jnp.sqrt(jnp.sum(jnp.sum(squares[...], axis=0), axis=1, keepdims=True))
    clip_scale = jnp.minimum(1.0, norm_limit / (norm + norm_eps))
    fresh, moment_next, variance_next = adam_update(
        summed[...], params[...], moment[...], variance[...], clip_scale
    )
    fresh_out[...] = fresh
    moment_out[...] = moment_next
    variance_out[...] = variance_next

    def rows(array, start):
        return jnp.concatenate(
            [array[first + row, :, start : start + width] for row in range(own_rows)], axis=0
        )

    groups = adam_update(
        rows(received, 0), rows(state, 0), rows(state, width), rows(state, 2 * width), clip_scale
    )[0]
    groups_out[...] = groups.astype(groups_out.dtype)


def shards(grads, params, moment, variance, save_owner):
    own_rows, width = params.shape
    tensor_count = lax.axis_size(TENSOR)
    far, core = lax.axis_index("dp_1"), lax.axis_index("dp_2")
    norm_limit = math.sqrt(float(grads.shape[1] * width * tensor_count))
    tile = jax.ShapeDtypeStruct((own_rows, width), jnp.float32)

    by_place = grads[0].reshape(
        lax.axis_size("dp_0"), lax.axis_size("dp_1"), lax.axis_size("dp_2"), own_rows, width
    )
    kept = lax.dynamic_index_in_dim(by_place, core, axis=2, keepdims=False)
    sent = lax.dynamic_index_in_dim(by_place, 1 - core, axis=2, keepdims=False)
    arrived = lax.ppermute(sent, "dp_2", SWAP)

    def pair_sum(side):
        return lax.dynamic_index_in_dim(kept, side, axis=1, keepdims=False).astype(
            jnp.float32
        ) + lax.dynamic_index_in_dim(arrived, side, axis=1, keepdims=False).astype(jnp.float32)

    params, moment, variance = map(keep, (params, moment, variance))
    state = pl.pallas_call(
        pack_state,
        out_shape=jax.ShapeDtypeStruct((tensor_count, 1, 3 * width), jnp.float32),
        in_specs=[in_smem()] + [in_vmem()] * 3,
        out_specs=in_vmem(),
    )(save_owner, params, moment, variance)
    state = exchange(state, TENSOR)

    code = encode(pair_sum(1 - far))
    code = lax.ppermute(code, "dp_1", SWAP)
    four = pair_sum(far) + decode(code)

    codes, state = lax.optimization_barrier((encode(four), state))
    summed = jnp.sum(decode(exchange(codes, "dp_0")), axis=0)

    pieces = pl.pallas_call(
        pack_summed,
        out_shape=pltpu.VMEM((tensor_count, 1, width + LANES), jnp.float32),
        in_specs=[in_smem(), in_vmem()],
        out_specs=in_vmem(),
    )(save_owner, keep(summed))
    received = exchange(pieces, TENSOR)
    squares = jnp.sum(received[:, :, width:], axis=0, keepdims=True)
    squares = exchange(jnp.broadcast_to(squares, (4, 1, LANES)), ("dp_1", "dp_2"))
    squares = jnp.sum(squares, axis=0, keepdims=True)
    squares = exchange(jnp.broadcast_to(squares, (12, 1, LANES)), "dp_0")

    return pl.pallas_call(
        functools.partial(finish, norm_limit),
        out_shape=(tile, tile, tile, jax.ShapeDtypeStruct(tile.shape, jnp.bfloat16)),
        in_specs=[in_smem()] + [in_vmem()] * 7,
        out_specs=[in_vmem()] * 4,
    )(save_owner, *map(keep, (squares, received, state, summed)), params, moment, variance)


def solution(mesh):
    torus = Mesh(
        mesh.devices.reshape(12, 2, 2, 8, 2), ("dp_0", "dp_1", "dp_2", "tensor_0", "tensor_1")
    )
    return jax.shard_map(
        shards,
        mesh=torus,
        in_specs=(P(DP, None, TENSOR), P(DP, TENSOR), P(DP, TENSOR), P(DP, TENSOR), P(DP, None)),
        out_specs=(P(DP, TENSOR), P(DP, TENSOR), P(DP, TENSOR), P(DP_TENSOR, None)),
        check_vma=False,
    )
```

```python
import functools
import math

import jax
import jax.numpy as jnp
from jax import lax
from jax.experimental import pallas as pl
from jax.experimental.pallas import tpu as pltpu
from jax.sharding import Mesh
from jax.sharding import PartitionSpec as P


TENSOR = ("tensor_0", "tensor_1")
DP = ("dp_0", "dp_1", "dp_2")
DP_TENSOR = ("dp_0", "dp_1", "dp_2", "tensor_0", "tensor_1")
SWAP = ((0, 1), (1, 0))
LANES = 128

learn_rate = 0.05
beta_first = 0.9
beta_second = 0.999
adam_step = 1000.0
adam_eps = 1e-08
norm_eps = 1e-06

SPREAD = 16.0


def encode(value):
    return (value * SPREAD).astype(jnp.float16)


def decode(code):
    return code.astype(jnp.float32) * (1.0 / SPREAD)


def adam_update(summed, params, moment, variance, clip_scale):
    scaled = clip_scale * summed
    moment_next = beta_first * moment + (1.0 - beta_first) * scaled
    variance_next = beta_second * variance + (1.0 - beta_second) * scaled * scaled
    first_fix = 1.0 - beta_first**adam_step
    second_fix = 1.0 - beta_second**adam_step
    update = moment_next / first_fix / (jnp.sqrt(variance_next / second_fix) + adam_eps)
    return (params - learn_rate * update, moment_next, variance_next)


def exchange(array, axes):
    return lax.all_to_all(array, axes, split_axis=0, concat_axis=0, tiled=True)


def in_vmem():
    return pl.BlockSpec(memory_space=pltpu.VMEM)


def keep(array):
    return pltpu.with_memory_space_constraint(array, pltpu.VMEM)


def in_smem():
    return pl.BlockSpec(memory_space=pltpu.SMEM)


def load(owners, grads, params, moment, variance, state, kept, sent, *rest):
    own_rows, width = params.shape
    halves = owners.shape[1] // own_rows
    half = lax.axis_index(TENSOR) // own_rows
    core = lax.axis_index("dp_2")
    own, semaphores = rest[:3], rest[3]
    copies = [
        pltpu.make_async_copy(array, place, semaphores.at[index])
        for index, (array, place) in enumerate(zip((params, moment, variance), own))
    ]
    for index, (place, whose) in enumerate(((sent, 1 - core), (kept, core))):
        for side in range(place.shape[0]):
            copies.append(
                pltpu.make_async_copy(
                    grads.at[:, side, whose],
                    place.at[side],
                    semaphores.at[3 + index * place.shape[0] + side],
                )
            )
    for copy in copies:
        copy.start()
    for place, array in enumerate(own):
        copies[place].wait()
        for row in range(own_rows):
            slot = owners[0, row * halves + half]
            state[slot, :, place * width : (place + 1) * width] = array[row : row + 1, :]
    for copy in copies[3:]:
        copy.wait()


def pack_summed(owners, summed, out):
    own_rows, width = summed.shape
    halves = owners.shape[1] // own_rows
    half = lax.axis_index(TENSOR) // own_rows
    squares = jnp.zeros((own_rows, LANES), jnp.float32)
    for start in range(0, width, LANES):
        tile = summed[:, start : start + LANES]
        squares = squares + tile * tile
    squares = jnp.sum(squares, axis=0, keepdims=True)
    for slot in range(out.shape[0]):
        out[slot, :, width:] = squares
    for row in range(own_rows):
        slot = owners[0, row * halves + half]
        out[slot, :, :width] = summed[row : row + 1, :]


def finish(norm_limit, owners, squares, received, state, summed, params, moment, variance,
           fresh_out, moment_out, variance_out, groups_out):
    own_rows, width = params.shape
    tensor_count = owners.shape[1]
    halves = tensor_count // own_rows
    place = lax.axis_index(TENSOR)
    first = jnp.int32(0)
    for group in range(tensor_count):
        first = jnp.where(owners[0, group] == place, group % halves * own_rows, first)
    norm = jnp.sqrt(jnp.sum(jnp.sum(squares[...], axis=0), axis=1, keepdims=True))
    clip_scale = jnp.minimum(1.0, norm_limit / (norm + norm_eps))
    fresh, moment_next, variance_next = adam_update(
        summed[...], params[...], moment[...], variance[...], clip_scale
    )
    fresh_out[...] = fresh
    moment_out[...] = moment_next
    variance_out[...] = variance_next

    def rows(array, start):
        return jnp.concatenate(
            [array[first + row, :, start : start + width] for row in range(own_rows)], axis=0
        )

    groups = adam_update(
        rows(received, 0), rows(state, 0), rows(state, width), rows(state, 2 * width), clip_scale
    )[0]
    groups_out[...] = groups.astype(groups_out.dtype)


def shards(grads, params, moment, variance, save_owner):
    own_rows, width = params.shape
    tensor_count = lax.axis_size(TENSOR)
    far = lax.axis_index("dp_1")
    norm_limit = math.sqrt(float(grads.shape[1] * width * tensor_count))
    tile = jax.ShapeDtypeStruct((own_rows, width), jnp.float32)

    by_place = grads[0].reshape(
        lax.axis_size("dp_0"), lax.axis_size("dp_1"), lax.axis_size("dp_2"), own_rows, width
    )
    core_count = lax.axis_size("dp_2")
    far_count = lax.axis_size("dp_1")
    part = pltpu.VMEM((far_count, by_place.shape[0], own_rows, width), grads.dtype)
    state, kept, sent, params, moment, variance = pl.pallas_call(
        load,
        out_shape=(
            jax.ShapeDtypeStruct((tensor_count, 1, 3 * width), jnp.float32),
            part,
            part,
            *[pltpu.VMEM(tile.shape, tile.dtype)] * 3,
        ),
        in_specs=[in_smem()] + [pl.BlockSpec(memory_space=pl.ANY)] * 4,
        out_specs=[in_vmem()] * 6,
        scratch_shapes=[pltpu.SemaphoreType.DMA((3 + far_count * core_count,))],
    )(save_owner, by_place, params, moment, variance)
    arrived = lax.ppermute(sent, "dp_2", SWAP)

    def pair_sum(side):
        return lax.dynamic_index_in_dim(kept, side, axis=0, keepdims=False).astype(
            jnp.float32
        ) + lax.dynamic_index_in_dim(arrived, side, axis=0, keepdims=False).astype(jnp.float32)

    state = exchange(state, TENSOR)

    code = encode(pair_sum(1 - far))
    code = lax.ppermute(code, "dp_1", SWAP)
    four = pair_sum(far) + decode(code)

    codes, state = lax.optimization_barrier((encode(four), state))
    summed = jnp.sum(decode(exchange(codes, "dp_0")), axis=0)

    pieces = pl.pallas_call(
        pack_summed,
        out_shape=pltpu.VMEM((tensor_count, 1, width + LANES), jnp.float32),
        in_specs=[in_smem(), in_vmem()],
        out_specs=in_vmem(),
    )(save_owner, keep(summed))
    received = exchange(pieces, TENSOR)
    squares = jnp.sum(received[:, :, width:], axis=0, keepdims=True)
    squares = exchange(jnp.broadcast_to(squares, (lax.axis_size(DP), 1, LANES)), DP)

    return pl.pallas_call(
        functools.partial(finish, norm_limit),
        out_shape=(tile, tile, tile, jax.ShapeDtypeStruct(tile.shape, jnp.bfloat16)),
        in_specs=[in_smem()] + [in_vmem()] * 7,
        out_specs=[in_vmem()] * 4,
    )(save_owner, *map(keep, (squares, received, state, summed, params, moment, variance)))


def solution(mesh):
    torus = Mesh(
        mesh.devices.reshape(12, 2, 2, 8, 2), ("dp_0", "dp_1", "dp_2", "tensor_0", "tensor_1")
    )
    return jax.shard_map(
        shards,
        mesh=torus,
        in_specs=(P(DP, None, TENSOR), P(DP, TENSOR), P(DP, TENSOR), P(DP, TENSOR), P(DP, None)),
        out_specs=(P(DP, TENSOR), P(DP, TENSOR), P(DP, TENSOR), P(DP_TENSOR, None)),
        check_vma=False,
    )
```

```python
import functools
import math

import jax
import jax.numpy as jnp
from jax import lax
from jax.experimental import pallas as pl
from jax.experimental.pallas import tpu as pltpu
from jax.sharding import Mesh
from jax.sharding import PartitionSpec as P


TENSOR = ("tensor_0", "tensor_1")
DP = ("dp_0", "dp_1", "dp_2")
DP_TENSOR = ("dp_0", "dp_1", "dp_2", "tensor_0", "tensor_1")
SWAP = ((0, 1), (1, 0))
LANES = 128

learn_rate = 0.05
beta_first = 0.9
beta_second = 0.999
adam_step = 1000.0
adam_eps = 1e-08
norm_eps = 1e-06

SPREAD = 16.0


def encode(value):
    return (value * SPREAD).astype(jnp.float16)


def decode(code):
    return code.astype(jnp.float32) * (1.0 / SPREAD)


def adam_update(summed, params, moment, variance, clip_scale):
    scaled = clip_scale * summed
    moment_next = beta_first * moment + (1.0 - beta_first) * scaled
    variance_next = beta_second * variance + (1.0 - beta_second) * scaled * scaled
    first_fix = 1.0 - beta_first**adam_step
    second_fix = 1.0 - beta_second**adam_step
    update = moment_next / first_fix / (jnp.sqrt(variance_next / second_fix) + adam_eps)
    return (params - learn_rate * update, moment_next, variance_next)


def exchange(array, axes):
    return lax.all_to_all(array, axes, split_axis=0, concat_axis=0, tiled=True)


def in_vmem():
    return pl.BlockSpec(memory_space=pltpu.VMEM)


def keep(array):
    return pltpu.with_memory_space_constraint(array, pltpu.VMEM)


def in_smem():
    return pl.BlockSpec(memory_space=pltpu.SMEM)


def load(grads, params, moment, variance, kept, sent, *rest):
    core = lax.axis_index("dp_2")
    own, semaphores = rest[:3], rest[3]
    copies = [
        pltpu.make_async_copy(array, place, semaphores.at[index])
        for index, (array, place) in enumerate(zip((params, moment, variance), own))
    ]
    for index, (place, whose) in enumerate(((sent, 1 - core), (kept, core))):
        for side in range(place.shape[0]):
            copies.append(
                pltpu.make_async_copy(
                    grads.at[:, side, whose],
                    place.at[side],
                    semaphores.at[3 + index * place.shape[0] + side],
                )
            )
    for copy in copies:
        copy.start()
    for copy in copies:
        copy.wait()


def pack_state(owners, params, moment, variance, out):
    own_rows, width = params.shape
    halves = owners.shape[1] // own_rows
    half = lax.axis_index(TENSOR) // own_rows
    for row in range(own_rows):
        slot = owners[0, row * halves + half]
        for place, array in enumerate((params, moment, variance)):
            start = (place + 1) * width
            out[slot, :, start : start + width] = array[row : row + 1, :]


def pack_summed(owners, summed, state, out):
    own_rows, width = summed.shape
    halves = owners.shape[1] // own_rows
    half = lax.axis_index(TENSOR) // own_rows
    squares = jnp.zeros((own_rows, LANES), jnp.float32)
    for start in range(0, width, LANES):
        tile = summed[:, start : start + LANES]
        squares = squares + tile * tile
    squares = jnp.sum(squares, axis=0, keepdims=True)
    for slot in range(out.shape[0]):
        out[slot, :, 4 * width :] = squares
    for row in range(own_rows):
        slot = owners[0, row * halves + half]
        out[slot, :, :width] = summed[row : row + 1, :]


def finish(norm_limit, owners, squares, received, summed, params, moment, variance,
           fresh_out, moment_out, variance_out, groups_out):
    own_rows, width = params.shape
    tensor_count = owners.shape[1]
    halves = tensor_count // own_rows
    place = lax.axis_index(TENSOR)
    first = jnp.int32(0)
    for group in range(tensor_count):
        first = jnp.where(owners[0, group] == place, group % halves * own_rows, first)
    norm = jnp.sqrt(jnp.sum(jnp.sum(squares[...], axis=0), axis=1, keepdims=True))
    clip_scale = jnp.minimum(1.0, norm_limit / (norm + norm_eps))
    fresh, moment_next, variance_next = adam_update(
        summed[...], params[...], moment[...], variance[...], clip_scale
    )
    fresh_out[...] = fresh
    moment_out[...] = moment_next
    variance_out[...] = variance_next

    def rows(place):
        start = place * width
        return jnp.concatenate(
            [received[first + row, :, start : start + width] for row in range(own_rows)], axis=0
        )

    groups = adam_update(*map(rows, range(4)), clip_scale)[0]
    groups_out[...] = groups.astype(groups_out.dtype)


def shards(grads, params, moment, variance, save_owner):
    own_rows, width = params.shape
    tensor_count = lax.axis_size(TENSOR)
    far = lax.axis_index("dp_1")
    norm_limit = math.sqrt(float(grads.shape[1] * width * tensor_count))
    tile = jax.ShapeDtypeStruct((own_rows, width), jnp.float32)

    by_place = grads[0].reshape(
        lax.axis_size("dp_0"), lax.axis_size("dp_1"), lax.axis_size("dp_2"), own_rows, width
    )
    core_count = lax.axis_size("dp_2")
    far_count = lax.axis_size("dp_1")
    part = pltpu.VMEM((far_count, by_place.shape[0], own_rows, width), grads.dtype)
    kept, sent, params, moment, variance = pl.pallas_call(
        load,
        out_shape=(
            part,
            part,
            *[pltpu.VMEM(tile.shape, tile.dtype)] * 3,
        ),
        in_specs=[pl.BlockSpec(memory_space=pl.ANY)] * 4,
        out_specs=[in_vmem()] * 5,
        scratch_shapes=[pltpu.SemaphoreType.DMA((3 + far_count * core_count,))],
    )(by_place, params, moment, variance)
    arrived = lax.ppermute(sent, "dp_2", SWAP)

    def pair_sum(side):
        return lax.dynamic_index_in_dim(kept, side, axis=0, keepdims=False).astype(
            jnp.float32
        ) + lax.dynamic_index_in_dim(arrived, side, axis=0, keepdims=False).astype(jnp.float32)

    piece = pltpu.VMEM((tensor_count, 1, 4 * width + LANES), jnp.float32)
    state = pl.pallas_call(
        pack_state,
        out_shape=piece,
        in_specs=[in_smem()] + [in_vmem()] * 3,
        out_specs=in_vmem(),
    )(save_owner, *map(keep, (params, moment, variance)))

    code = encode(pair_sum(1 - far))
    code = lax.ppermute(code, "dp_1", SWAP)
    four = pair_sum(far) + decode(code)

    summed = jnp.sum(decode(exchange(encode(four), "dp_0")), axis=0)

    pieces = pl.pallas_call(
        pack_summed,
        out_shape=piece,
        in_specs=[in_smem(), in_vmem(), in_vmem()],
        out_specs=in_vmem(),
        input_output_aliases={2: 0},
    )(save_owner, keep(summed), keep(state))
    received = exchange(pieces, TENSOR)
    squares = jnp.sum(received[:, :, 4 * width :], axis=0, keepdims=True)
    squares = exchange(jnp.broadcast_to(squares, (lax.axis_size(DP), 1, LANES)), DP)

    return pl.pallas_call(
        functools.partial(finish, norm_limit),
        out_shape=(tile, tile, tile, jax.ShapeDtypeStruct(tile.shape, jnp.bfloat16)),
        in_specs=[in_smem()] + [in_vmem()] * 6,
        out_specs=[in_vmem()] * 4,
    )(save_owner, *map(keep, (squares, received, summed, params, moment, variance)))


def solution(mesh):
    torus = Mesh(
        mesh.devices.reshape(12, 2, 2, 8, 2), ("dp_0", "dp_1", "dp_2", "tensor_0", "tensor_1")
    )
    return jax.shard_map(
        shards,
        mesh=torus,
        in_specs=(P(DP, None, TENSOR), P(DP, TENSOR), P(DP, TENSOR), P(DP, TENSOR), P(DP, None)),
        out_specs=(P(DP, TENSOR), P(DP, TENSOR), P(DP, TENSOR), P(DP_TENSOR, None)),
        check_vma=False,
    )
```

```python
import functools
import math

import jax
import jax.numpy as jnp
from jax import lax
from jax.experimental import pallas as pl
from jax.experimental.pallas import tpu as pltpu
from jax.sharding import Mesh
from jax.sharding import PartitionSpec as P


TENSOR = ("tensor_0", "tensor_1")
DP = ("dp_0", "dp_1", "dp_2")
DP_TENSOR = ("dp_0", "dp_1", "dp_2", "tensor_0", "tensor_1")
SWAP = ((0, 1), (1, 0))
LANES = 128

learn_rate = 0.05
beta_first = 0.9
beta_second = 0.999
adam_step = 1000.0
adam_eps = 1e-08
norm_eps = 1e-06

SPREAD = 16.0


def encode(value):
    return (value * SPREAD).astype(jnp.float16)


def decode(code):
    return code.astype(jnp.float32) * (1.0 / SPREAD)


def adam_update(summed, params, moment, variance, clip_scale):
    scaled = clip_scale * summed
    moment_next = beta_first * moment + (1.0 - beta_first) * scaled
    variance_next = beta_second * variance + (1.0 - beta_second) * scaled * scaled
    first_fix = 1.0 - beta_first**adam_step
    second_fix = 1.0 - beta_second**adam_step
    update = moment_next / first_fix / (jnp.sqrt(variance_next / second_fix) + adam_eps)
    return (params - learn_rate * update, moment_next, variance_next)


def exchange(array, axes):
    return lax.all_to_all(array, axes, split_axis=0, concat_axis=0, tiled=True)


def in_vmem():
    return pl.BlockSpec(memory_space=pltpu.VMEM)


def keep(array):
    return pltpu.with_memory_space_constraint(array, pltpu.VMEM)


def in_smem():
    return pl.BlockSpec(memory_space=pltpu.SMEM)


def load_first(grads, out, semaphore):
    far, core = lax.axis_index("dp_1"), lax.axis_index("dp_2")
    copy = pltpu.make_async_copy(grads.at[:, 1 - far, 1 - core], out, semaphore)
    copy.start()
    copy.wait()


def load_rest(grads, params, moment, variance, sent, kept_first, kept_rest, *rest):
    far, core = lax.axis_index("dp_1"), lax.axis_index("dp_2")
    semaphores = rest[3]
    pairs = (
        (grads.at[:, 1 - far, core], kept_first),
        (grads.at[:, far, 1 - core], sent),
        (grads.at[:, far, core], kept_rest),
        *zip((params, moment, variance), rest[:3]),
    )
    copies = [
        pltpu.make_async_copy(source, place, semaphores.at[index])
        for index, (source, place) in enumerate(pairs)
    ]
    for copy in copies:
        copy.start()
    for copy in copies:
        copy.wait()


def pack_state(owners, params, moment, variance, out):
    own_rows, width = params.shape
    halves = owners.shape[1] // own_rows
    half = lax.axis_index(TENSOR) // own_rows
    for row in range(own_rows):
        slot = owners[0, row * halves + half]
        for place, array in enumerate((params, moment, variance)):
            start = (place + 1) * width
            out[slot, :, start : start + width] = array[row : row + 1, :]


def pack_summed(owners, summed, state, out, held_owners, semaphore):
    own_rows, width = summed.shape
    copy = pltpu.make_async_copy(owners, held_owners, semaphore)
    copy.start()
    halves = owners.shape[1] // own_rows
    half = lax.axis_index(TENSOR) // own_rows
    squares = jnp.zeros((own_rows, LANES), jnp.float32)
    for start in range(0, width, LANES):
        tile = summed[:, start : start + LANES]
        squares = squares + tile * tile
    squares = jnp.sum(squares, axis=0, keepdims=True)
    for slot in range(out.shape[0]):
        out[slot, :, 4 * width :] = squares
    copy.wait()
    for row in range(own_rows):
        slot = held_owners[0, row * halves + half]
        out[slot, :, :width] = summed[row : row + 1, :]


def finish(norm_limit, owners, squares, received, summed, params, moment, variance, *rest):
    outs, held, held_owners, semaphores = rest[:4], rest[4:8], rest[8], rest[9]
    own_rows, width = params.shape
    tensor_count = owners.shape[1]
    halves = tensor_count // own_rows
    owners_copy = pltpu.make_async_copy(owners, held_owners, semaphores.at[4])
    owners_copy.start()
    copies = [
        pltpu.make_async_copy(source, out, semaphores.at[index])
        for index, (source, out) in enumerate(zip(held, outs))
    ]
    norm = jnp.sqrt(jnp.sum(jnp.sum(squares[...], axis=0), axis=1, keepdims=True))
    clip_scale = jnp.minimum(1.0, norm_limit / (norm + norm_eps))
    results = adam_update(summed[...], params[...], moment[...], variance[...], clip_scale)
    for copy, place, result in zip(copies, held, results):
        place[...] = result
        copy.start()

    owners_copy.wait()
    place = lax.axis_index(TENSOR)
    first = jnp.int32(0)
    for group in range(tensor_count):
        first = jnp.where(held_owners[0, group] == place, group % halves * own_rows, first)

    def rows(place):
        start = place * width
        return jnp.concatenate(
            [received[first + row, :, start : start + width] for row in range(own_rows)], axis=0
        )

    groups = adam_update(*map(rows, range(4)), clip_scale)[0]
    held[3][...] = groups.astype(held[3].dtype)
    copies[3].start()
    for copy in copies:
        copy.wait()


def shards(grads, params, moment, variance, save_owner):
    own_rows, width = params.shape
    tensor_count = lax.axis_size(TENSOR)
    norm_limit = math.sqrt(float(grads.shape[1] * width * tensor_count))
    tile = jax.ShapeDtypeStruct((own_rows, width), jnp.float32)

    by_place = grads[0].reshape(
        lax.axis_size("dp_0"), lax.axis_size("dp_1"), lax.axis_size("dp_2"), own_rows, width
    )
    part = pltpu.VMEM((by_place.shape[0], own_rows, width), grads.dtype)
    in_hbm = pl.BlockSpec(memory_space=pl.ANY)

    sent = pl.pallas_call(
        load_first,
        out_shape=part,
        in_specs=[in_hbm],
        out_specs=in_vmem(),
        scratch_shapes=[pltpu.SemaphoreType.DMA(())],
    )(by_place)
    arrived_first = lax.ppermute(sent, "dp_2", SWAP)
    sent, kept_first, kept_rest, params, moment, variance = pl.pallas_call(
        load_rest,
        out_shape=(*[part] * 3, *[pltpu.VMEM(tile.shape, tile.dtype)] * 3),
        in_specs=[in_hbm] * 4,
        out_specs=[in_vmem()] * 6,
        scratch_shapes=[pltpu.SemaphoreType.DMA((6,))],
    )(by_place, params, moment, variance)
    arrived_rest = lax.ppermute(sent, "dp_2", SWAP)

    def pair_sum(kept, arrived):
        return kept.astype(jnp.float32) + arrived.astype(jnp.float32)

    piece = pltpu.VMEM((tensor_count, 1, 4 * width + LANES), jnp.float32)
    state = pl.pallas_call(
        pack_state,
        out_shape=piece,
        in_specs=[in_smem()] + [in_vmem()] * 3,
        out_specs=in_vmem(),
    )(save_owner, *map(keep, (params, moment, variance)))

    code = encode(pair_sum(kept_first, arrived_first))
    code = lax.ppermute(code, "dp_1", SWAP)
    four = pair_sum(kept_rest, arrived_rest) + decode(code)

    summed = jnp.sum(decode(exchange(encode(four), "dp_0")), axis=0)

    pieces = pl.pallas_call(
        pack_summed,
        out_shape=piece,
        in_specs=[in_hbm, in_vmem(), in_vmem()],
        out_specs=in_vmem(),
        scratch_shapes=[pltpu.SMEM(save_owner.shape, jnp.int32), pltpu.SemaphoreType.DMA(())],
        input_output_aliases={2: 0},
    )(save_owner, keep(summed), keep(state))
    received = exchange(pieces, TENSOR)
    squares = jnp.sum(received[:, :, 4 * width :], axis=0, keepdims=True)
    squares = exchange(jnp.broadcast_to(squares, (lax.axis_size(DP), 1, LANES)), DP)

    outs = [tile, tile, tile, jax.ShapeDtypeStruct(tile.shape, jnp.bfloat16)]
    return pl.pallas_call(
        functools.partial(finish, norm_limit),
        out_shape=outs,
        in_specs=[in_hbm] + [in_vmem()] * 6,
        out_specs=[in_hbm] * 4,
        scratch_shapes=[
            *[pltpu.VMEM(out.shape, out.dtype) for out in outs],
            pltpu.SMEM(save_owner.shape, jnp.int32),
            pltpu.SemaphoreType.DMA((5,)),
        ],
    )(save_owner, *map(keep, (squares, received, summed, params, moment, variance)))


def solution(mesh):
    torus = Mesh(
        mesh.devices.reshape(12, 2, 2, 8, 2), ("dp_0", "dp_1", "dp_2", "tensor_0", "tensor_1")
    )
    return jax.shard_map(
        shards,
        mesh=torus,
        in_specs=(P(DP, None, TENSOR), P(DP, TENSOR), P(DP, TENSOR), P(DP, TENSOR), P(DP, None)),
        out_specs=(P(DP, TENSOR), P(DP, TENSOR), P(DP, TENSOR), P(DP_TENSOR, None)),
        check_vma=False,
    )
```
